128 devices in a mesh: member: 64 (over y_hi, z, x, core), cell: 2 (over y_lo).
Axes of the slice: x: 4, y: 4 (y_hi: 2, y_lo: 2; y = y_hi * 2 + y_lo), z: 4, core: 2. Of those that a mesh axis runs over, the one named last changes fastest.
Arguments:
- background_physical: bfloat16 [64, 128, 192, 384], P('member', None, 'cell'), may hold values from -6 to 6
- probe_surface_harmonic: int32 [2048], replicated, may hold values from 0 to 49151
- reading_destination_part: int32 [2048], replicated, may hold values from 0 to 63
- observed_readings: float32 [2048], replicated, may hold values from -8 to 8
- reading_spread: float32 [2048], replicated, may hold values from 0.5 to 2
- harmonic_update_weight: float32 [192, 384], P('cell'), may hold values from 0.1 to 1
Outputs:
- increments: bfloat16 [64, 128, 192, 384], P('member', None, 'cell')
The draws below stay inside these ranges and needn't reach their ends.
Inputs may be any that keep to these rules, and one draw needn't show every extreme that they name: `probe_surface_harmonic`: the index a * 384 + k of axial plane a and circumferential Fourier mode k. `reading_destination_part`: block b covers axial planes b * 2 to (b + 1) * 2 - 1.
All inputs are finite; a program needn't handle non-finite values.
Results may differ from the reference program's by a relative error of at most 0.0098.
Values may be sent and summed in bfloat16 or wider, within the bound.
A program may use at most 128 MiB of HBM per device.

```python
import math
import jax
import jax.numpy as jnp
from jax import lax

ANGULAR_NODES = 384
RADIUS_TIERS = 192
SENS = 2048
NS_ITERS = 24
DOWNSTREAM_CUTS = 128
MEMBER_NUMBER = 64
BLOCKS = 64
N_MEMBER = 64


def set_ends(drawn, stream_key, smallest, high):
    spot = [jax.random.randint(jax.random.fold_in(stream_key, axis), (), 0, length) for axis, length in enumerate(drawn.shape)]
    main_axis = drawn.shape.index(max(drawn.shape))
    neighbour = spot[:main_axis] + [(spot[main_axis] + 1) % drawn.shape[main_axis]] + spot[main_axis + 1:]
    return drawn.at[tuple(spot)].set(smallest).at[tuple(neighbour)].set(high)


def level_of(rng, shape, split, smallest, top_value):
    def one(axis_at, blocks):
        steps = jax.random.uniform(jax.random.fold_in(jax.random.fold_in(rng, 6), axis_at), (blocks,), jnp.float32, smallest / len(split), top_value / len(split))
        return jnp.repeat(jnp.exp(steps), shape[axis_at] // blocks).reshape((-1,) + (1,) * (len(shape) - axis_at - 1))

    gain = one(*split[0])
    for cut in split[1:]:
        gain = gain * one(*cut)
    return gain


def noise(stream_key, extent, width, most, shards=(), held_as=jnp.bfloat16):
    loudness = level_of(stream_key, extent, shards, -0.22, 0.18) if shards else 1.0
    entries = jax.random.normal(stream_key, extent, jnp.float32) * width * loudness
    return jnp.minimum(jnp.maximum(entries, -most), most).astype(held_as)


def setup_inputs(seed: int = 0) -> dict:
    seeds = jax.random.split(jax.random.key(seed), 7)
    background_physical = noise(seeds[0], (MEMBER_NUMBER, DOWNSTREAM_CUTS, RADIUS_TIERS, ANGULAR_NODES), 1.0, 6.0, ((0, 64), (2, 2)))
    probe_surface_harmonic = set_ends(jax.random.randint(seeds[1], (SENS,), 0, DOWNSTREAM_CUTS * ANGULAR_NODES), jax.random.fold_in(seeds[1], 1), 0, (DOWNSTREAM_CUTS * ANGULAR_NODES) - 1).astype(jnp.int32)
    reading_destination_part = set_ends(jax.random.randint(seeds[2], (SENS,), 0, BLOCKS), jax.random.fold_in(seeds[2], 1), 0, BLOCKS - 1).astype(jnp.int32)
    observed_readings = noise(seeds[3], (SENS,), 2.0, 8.0, (), jnp.float32)
    reading_spread = jnp.clip(jnp.exp(jax.random.uniform(seeds[4], (SENS,), jnp.float32, math.log(0.5), math.log(2.0))), 0.5, 2.0)
    harmonic_update_weight = jnp.clip(jnp.exp(math.log(1.0) - 2.3025851 * jax.random.uniform(seeds[5], (RADIUS_TIERS, ANGULAR_NODES), jnp.float32) ** level_of(seeds[5], (RADIUS_TIERS, ANGULAR_NODES), ((0, 2),), -0.2, 0.2)), 0.1, 1.0)
    return {"background_physical": background_physical, "probe_surface_harmonic": probe_surface_harmonic, "reading_destination_part": reading_destination_part, "observed_readings": observed_readings, "reading_spread": reading_spread, "harmonic_update_weight": harmonic_update_weight}


def dft_basis(length):
    row_index = lax.broadcasted_iota(jnp.int32, (length, length), 0)
    col_index = lax.broadcasted_iota(jnp.int32, (length, length), 1)
    half_len = length // 2
    frequency = jnp.where(col_index <= half_len, col_index, col_index - half_len)
    product_mod = row_index * frequency % length
    phase_angle = 2.0 * jnp.pi * product_mod.astype(jnp.float32) / length
    basis_vals = jnp.where(col_index <= half_len, jnp.cos(phase_angle), jnp.sin(phase_angle))
    edge_cols = (col_index == 0) | (col_index == half_len)
    norm_factor = jnp.where(edge_cols, jnp.sqrt(1.0 / length), jnp.sqrt(2.0 / length))
    return (basis_vals * norm_factor).astype(jnp.bfloat16)

def mapping_operator(expected_readings, observed_readings, reading_spread, reading_destination_part, assigned_partition, member_number):
    observed_anomalies = lax.Precision.HIGHEST
    unit_diagonal = jnp.eye(member_number, dtype=jnp.float32)
    pred_mean = lax.optimization_barrier(jnp.mean(expected_readings, axis=1))
    anomaly = expected_readings - pred_mean[:, None]
    selector = (reading_destination_part == assigned_partition).astype(jnp.float32) / reading_spread
    normalized_anomaly = anomaly * selector[:, None]
    innovation = (observed_readings - pred_mean) * selector
    inner_product_grid = (member_number - 1.0) * unit_diagonal + jnp.dot(normalized_anomaly.T, normalized_anomaly, precision=observed_anomalies)
    right_term = jnp.dot(normalized_anomaly.T, innovation, precision=observed_anomalies)
    norm_scale = jnp.sqrt(jnp.sum(inner_product_grid * inner_product_grid))

    def newton_iter(count, carry):
        iterate, inv_root = carry
        newton_step = 1.5 * unit_diagonal - 0.5 * jnp.dot(inv_root, iterate, precision=observed_anomalies)
        return (jnp.dot(iterate, newton_step, precision=observed_anomalies), jnp.dot(newton_step, inv_root, precision=observed_anomalies))
    iterate, inv_root = lax.fori_loop(0, NS_ITERS, newton_iter, (inner_product_grid / norm_scale, unit_diagonal))
    reciprocal_root = inv_root / jnp.sqrt(norm_scale)
    inv_gram = jnp.dot(reciprocal_root, reciprocal_root, precision=observed_anomalies)
    combination_factors = jnp.dot(inv_gram, right_term, precision=observed_anomalies)
    merged_product = combination_factors[:, None] + jnp.sqrt(member_number - 1.0) * reciprocal_root
    mean_removal = unit_diagonal - 1.0 / member_number
    complete_lookup = 1.0 / member_number + jnp.dot(mean_removal, merged_product, precision=observed_anomalies)
    return (complete_lookup - unit_diagonal).astype(jnp.bfloat16)

def reference(background_physical, probe_surface_harmonic, reading_destination_part, observed_readings, reading_spread, harmonic_update_weight):
    member_number = background_physical.shape[0]
    trigonometric_design = dft_basis(ANGULAR_NODES)
    surface_field_entries = background_physical[:, :, RADIUS_TIERS - 2:, :].reshape(-1, ANGULAR_NODES)
    boundary_coefficients = jnp.dot(surface_field_entries, trigonometric_design, preferred_element_type=jnp.float32).astype(jnp.bfloat16)
    boundary_coefficients = boundary_coefficients.reshape(member_number, DOWNSTREAM_CUTS, 2, ANGULAR_NODES).astype(jnp.float32)
    boundary_innovation = (boundary_coefficients[:, :, 1, :] - boundary_coefficients[:, :, 0, :]).reshape(member_number, DOWNSTREAM_CUTS * ANGULAR_NODES)
    expected_readings = boundary_innovation[:, probe_surface_harmonic].T
    downstream_cuts = DOWNSTREAM_CUTS // N_MEMBER

    def one_block(assigned_partition):
        blend_coefficients = mapping_operator(expected_readings, observed_readings, reading_spread, reading_destination_part, assigned_partition, member_number)
        leading_shift = (assigned_partition * downstream_cuts).astype(jnp.int32)
        predicted_layouts = lax.dynamic_slice_in_dim(background_physical, leading_shift, downstream_cuts, 1)
        spectral_coefficients = jnp.dot(predicted_layouts.reshape(-1, ANGULAR_NODES), trigonometric_design, preferred_element_type=jnp.float32)
        spectral_coefficients = spectral_coefficients.astype(jnp.bfloat16).reshape(member_number, downstream_cuts, RADIUS_TIERS, ANGULAR_NODES)
        changed = jnp.einsum('ij,iabc->jabc', blend_coefficients.astype(jnp.float32), spectral_coefficients.astype(jnp.float32))
        changed = (changed * harmonic_update_weight[None, None]).astype(jnp.bfloat16)
        final_output = jnp.dot(changed.reshape(-1, ANGULAR_NODES), trigonometric_design.T, preferred_element_type=jnp.float32)
        return final_output.astype(jnp.bfloat16).reshape(member_number, downstream_cuts, RADIUS_TIERS, ANGULAR_NODES)
    produced_pieces = lax.map(one_block, jnp.arange(N_MEMBER, dtype=jnp.int32))
    return jnp.transpose(produced_pieces, (1, 0, 2, 3, 4)).reshape(member_number, DOWNSTREAM_CUTS, RADIUS_TIERS, ANGULAR_NODES)
```

```python
import functools

import jax
import jax.numpy as jnp
import numpy as np
from jax import lax
from jax.experimental import pallas as pl
from jax.experimental.pallas import tpu as pltpu
from jax.sharding import PartitionSpec as P

NS_ITERS = 24
TILE = 16
LEAD = 2
STRIDE = 27
NT = (((1,), (1,)), ((), ()))


def dft_basis(length):
    rows = np.arange(length)[:, None]
    cols = np.arange(length)[None, :]
    half = length // 2
    frequency = np.where(cols <= half, cols, cols - half)
    phase = 2.0 * np.pi * (rows * frequency % length) / length
    table = np.where(cols <= half, np.cos(phase), np.sin(phase))
    edge = (cols == 0) | (cols == half)
    return (table * np.where(edge, np.sqrt(1.0 / length), np.sqrt(2.0 / length))).astype(np.float32)


def iota(shape, dim):
    return lax.broadcasted_iota(jnp.int32, shape, dim)


def eye(size):
    return (iota((size, size), 0) == iota((size, size), 1)).astype(jnp.float32)


def partner(me, k, members):
    offset = (k * STRIDE) % members
    core = (me % 2 + offset % 2) % 2
    x = ((me // 2) % 4 + (offset // 2) % 4) % 4
    z = ((me // 8) % 4 + (offset // 8) % 4) % 4
    y = (me // 32 + offset // 32) % 2
    return ((y * 4 + z) * 4 + x) * 2 + core


def thirds(a):
    first = a.astype(jnp.bfloat16)
    rest = a - first.astype(jnp.float32)
    second = rest.astype(jnp.bfloat16)
    return first, second, (rest - second.astype(jnp.float32)).astype(jnp.bfloat16)


def left_of(a):
    first, second, third = thirds(a)
    return jnp.concatenate([third, second, first, second, first, first], axis=1)


def product(a, b):
    first, second, third = thirds(b)
    right = jnp.concatenate([first, second, third, first, second, first], axis=0)
    return jnp.dot(left_of(a), right, preferred_element_type=jnp.float32)


def product_nt(a, b):
    first, second, third = thirds(b)
    right = jnp.concatenate([first, second, third, first, second, first], axis=1)
    return lax.dot_general(left_of(a), right, NT, preferred_element_type=jnp.float32)


def own_predictions(wall_ref, basis_t_ref, probe_ref, own_ref):
    planes, tile, modes = wall_ref.shape
    rows = planes * tile
    picked = iota((2 * planes, rows), 0)
    wanted = jnp.where(picked < planes, picked * tile + (tile - 1), (picked - planes) * tile + (tile - 2))
    pick = (iota((2 * planes, rows), 1) == wanted).astype(jnp.bfloat16)
    levels = jnp.dot(pick, wall_ref[...].reshape(rows, modes), preferred_element_type=jnp.float32)
    spectra_t = lax.dot_general(
        basis_t_ref[...], levels.astype(jnp.bfloat16), NT, preferred_element_type=jnp.float32
    ).astype(jnp.bfloat16)
    groups, width = own_ref.shape
    for g in range(groups):
        probe = probe_ref[:, g * width : (g + 1) * width]
        plane = ((probe >> 7) * 171) >> 9
        mode = probe - plane * modes
        row = iota((2 * planes, width), 0)
        sign = jnp.where(row == plane, 1.0, 0.0) - jnp.where(row == plane + planes, 1.0, 0.0)
        shear = jnp.dot(spectra_t, sign.astype(jnp.bfloat16), preferred_element_type=jnp.float32)
        taken = jnp.where(iota((modes, width), 0) == mode, shear, 0.0)
        own_ref[g : g + 1, :] = jnp.sum(taken, axis=0, keepdims=True)


def mixing_matrix(preds_ref, observed_ref, spread_ref, part_ref, block):
    members, groups, width = preds_ref.shape
    side = 128
    inside = (iota((side, side), 0) < members) & (iota((side, side), 1) < members)
    unit = eye(side) * inside.astype(jnp.float32)
    gram = (members - 1.0) * unit
    right = jnp.zeros((1, side), jnp.float32)
    empty = jnp.zeros((side - members, width), jnp.float32)
    for g in range(groups):
        lanes = slice(g * width, (g + 1) * width)
        preds = preds_ref[:, g, :]
        mean = jnp.sum(preds, axis=0, keepdims=True) * (1.0 / members)
        selector = jnp.where(part_ref[:, lanes] == block, 1.0, 0.0) / spread_ref[:, lanes]
        scaled = jnp.concatenate([(preds - mean) * selector, empty], axis=0)
        innovation = (observed_ref[:, lanes] - mean) * selector
        gram += product_nt(scaled, scaled)
        right += product_nt(jnp.broadcast_to(innovation, (16, width)), scaled)[:1]
    squares = jnp.sum(jnp.sum(gram * gram, axis=1, keepdims=True), axis=0, keepdims=True)
    norm = jnp.sqrt(squares)

    def newton_iter(count, carry):
        iterate, inv_root = carry
        step = 1.5 * unit - 0.5 * product(inv_root, iterate)
        return product(iterate, step), product(step, inv_root)

    _, inv_root = lax.fori_loop(0, NS_ITERS, newton_iter, (gram / norm, unit))
    root = inv_root / jnp.sqrt(norm)
    inv_gram = product(root, root)
    factors = jnp.sum(inv_gram * right, axis=1, keepdims=True)
    combined = factors + np.float32(np.sqrt(members - 1.0)) * root
    combined = jnp.where(inside, combined, 0.0)
    centred = combined - jnp.sum(combined, axis=0, keepdims=True) * (1.0 / members)
    return jnp.where(inside, (1.0 / members) + centred - unit, 0.0).astype(jnp.bfloat16)


def kernel(
    members,
    x_ref,
    basis_ref,
    basis_t_ref,
    probe_ref,
    part_ref,
    observed_ref,
    spread_ref,
    weight_ref,
    out_ref,
    wall,
    held,
    done,
    own,
    preds,
    spread_mix,
    spectra,
    wall_sem,
    give_sem,
    hold_sem,
    own_send,
    own_recv,
    preds_send,
    preds_recv,
    back_send,
    back_recv,
):
    chunks = held.shape[0]
    deep = held.shape[2]
    me = lax.axis_index("member")
    cell = lax.axis_index("cell")
    at_wall = cell == 1
    barrier = pltpu.get_barrier_semaphore()

    wall_copy = pltpu.make_async_copy(x_ref.at[0, :, pl.ds((chunks - 1) * TILE, TILE)], wall, wall_sem)
    wall_copy.start()

    @pl.loop(1, members)
    def _(k):
        pl.semaphore_signal(barrier, inc=1, device_id={"member": (me + k) % members})

    pl.semaphore_signal(barrier, inc=1, device_id={"cell": 1 - cell})
    pl.semaphore_wait(barrier, members)

    def give(c):
        rows = pl.ds(c * TILE, TILE)
        pltpu.make_async_copy(
            x_ref.at[0, pl.ds(me * deep, deep), rows], held.at[c, me], hold_sem.at[c]
        ).start()

        @pl.loop(1, members)
        def _(k):
            p = partner(me, k, members)
            pltpu.make_async_remote_copy(
                src_ref=x_ref.at[0, pl.ds(p * deep, deep), rows],
                dst_ref=held.at[c, me],
                send_sem=give_sem,
                recv_sem=hold_sem.at[c],
                device_id={"member": p},
            ).start()

    for c in range(LEAD):
        give(c)

    wall_copy.wait()
    to_sibling = pltpu.make_async_remote_copy(
        src_ref=own, dst_ref=own, send_sem=own_send, recv_sem=own_recv, device_id={"cell": 0}
    )

    @pl.when(at_wall)
    def _():
        own_predictions(wall, basis_t_ref, probe_ref, own)
        to_sibling.start()
        to_sibling.wait_send()

    @pl.when(jnp.logical_not(at_wall))
    def _():
        to_sibling.wait_recv()

    pltpu.make_async_copy(own, preds.at[me], preds_recv).start()

    @pl.loop(1, members)
    def _(k):
        pltpu.make_async_remote_copy(
            src_ref=own,
            dst_ref=preds.at[me],
            send_sem=preds_send,
            recv_sem=preds_recv,
            device_id={"member": partner(me, k, members)},
        ).start()

    @pl.loop(LEAD, chunks)
    def _(c):
        give(c)

    pltpu.make_async_copy(preds, preds, preds_recv).wait()
    mixing = mixing_matrix(preds, observed_ref, spread_ref, part_ref, me)

    wide = members * TILE
    high = 128
    across = (iota((high, wide), 1) // TILE == iota((high, wide), 0)).astype(jnp.bfloat16)

    @pl.loop(0, wide // high)
    def _(b):
        member = (iota((high, high), 0) + b * high) // TILE
        down = (member == iota((high, high), 1)).astype(jnp.bfloat16)
        part = lax.dot_general(down, mixing, NT, preferred_element_type=jnp.float32).astype(jnp.bfloat16)
        full = jnp.dot(part, across, preferred_element_type=jnp.float32)
        same = iota((high, wide), 0) % TILE == iota((high, wide), 1) % TILE
        spread_mix[pl.ds(pl.multiple_of(b * high, high), high), :] = jnp.where(same, full, 0.0).astype(jnp.bfloat16)

    step = 256
    some = step // TILE

    @pl.loop(0, chunks)
    def _(c):
        pltpu.make_async_copy(held.at[c], held.at[c], hold_sem.at[c]).wait()
        rows = pl.ds(pl.multiple_of(c * TILE, TILE), TILE)

        @pl.loop(0, deep)
        def _(p):
            @pl.loop(0, wide // step)
            def _(b):
                field = held[c, pl.ds(b * some, some), p].reshape(step, -1)
                spectra[pl.ds(pl.multiple_of(b * step, step), step), :] = jnp.dot(
                    field, basis_ref[...], preferred_element_type=jnp.float32
                ).astype(jnp.bfloat16)

            @pl.loop(0, wide // step)
            def _(b):
                changed = jnp.dot(
                    spread_mix[pl.ds(pl.multiple_of(b * step, step), step), :],
                    spectra[...],
                    preferred_element_type=jnp.float32,
                )
                changed = changed.reshape(some, TILE, -1) * weight_ref[rows, :][None]
                changed = changed.astype(jnp.bfloat16).reshape(step, -1)
                back = jnp.dot(changed, basis_t_ref[...], preferred_element_type=jnp.float32)
                done[c, pl.ds(b * some, some), p] = back.astype(jnp.bfloat16).reshape(some, TILE, -1)

        pltpu.make_async_copy(
            done.at[c, me], out_ref.at[0, pl.ds(me * deep, deep), rows], back_recv
        ).start()

        @pl.loop(1, members)
        def _(k):
            p = partner(me, k, members)
            pltpu.make_async_remote_copy(
                src_ref=done.at[c, p],
                dst_ref=out_ref.at[0, pl.ds(me * deep, deep), rows],
                send_sem=back_send,
                recv_sem=back_recv,
                device_id={"member": p},
            ).start()

    others = pl.ds(0, members - 1)
    pltpu.make_async_copy(preds.at[others], preds.at[others], preds_send).wait()
    pltpu.make_async_copy(held.at[:, others], held.at[:, others], give_sem).wait()
    pltpu.make_async_copy(held.at[:, others], held.at[:, others], back_send).wait()
    pltpu.make_async_copy(out_ref, out_ref, back_recv).wait()


def on_device(members, x, probe, part, observed, spread, weight):
    _, planes, levels, modes = x.shape
    sensors = probe.shape[0]
    chunks = levels // TILE
    deep = planes // members
    table = dft_basis(modes)
    basis = jnp.asarray(table, jnp.bfloat16)
    basis_t = jnp.asarray(table.T, jnp.bfloat16)
    vmem = pl.BlockSpec(memory_space=pltpu.VMEM)
    anywhere = pl.BlockSpec(memory_space=pl.ANY)
    dma = pltpu.SemaphoreType.DMA(())
    return pl.pallas_call(
        functools.partial(kernel, members),
        out_shape=jax.ShapeDtypeStruct(x.shape, x.dtype),
        in_specs=[anywhere] + [vmem] * 7,
        out_specs=anywhere,
        scratch_shapes=[
            pltpu.VMEM((planes, TILE, modes), jnp.bfloat16),
            pltpu.VMEM((chunks, members, deep, TILE, modes), jnp.bfloat16),
            pltpu.VMEM((chunks, members, deep, TILE, modes), jnp.bfloat16),
            pltpu.VMEM((8, sensors // 8), jnp.float32),
            pltpu.VMEM((members, 8, sensors // 8), jnp.float32),
            pltpu.VMEM((members * TILE, members * TILE), jnp.bfloat16),
            pltpu.VMEM((members * TILE, modes), jnp.bfloat16),
            dma,
            dma,
            pltpu.SemaphoreType.DMA((chunks,)),
            dma,
            dma,
            dma,
            dma,
            dma,
            dma,
        ],
        compiler_params=pltpu.CompilerParams(
            collective_id=0, has_side_effects=True, vmem_limit_bytes=48 << 20
        ),
    )(x, basis, basis_t, probe[None], part[None], observed[None], spread[None], weight)


def solution(mesh):
    return jax.shard_map(
        functools.partial(on_device, mesh.shape["member"]),
        mesh=mesh,
        in_specs=(P("member", None, "cell", None), P(), P(), P(), P(), P("cell", None)),
        out_specs=P("member", None, "cell", None),
        check_vma=False,
    )
```

```python
import functools

import jax
import jax.numpy as jnp
import numpy as np
from jax import lax
from jax.experimental import pallas as pl
from jax.experimental.pallas import tpu as pltpu
from jax.sharding import PartitionSpec as P

NS_ITERS = 24
STRIDE = 37
TILE = 16
LEAD = 3
NT = (((1,), (1,)), ((), ()))


def dft_basis(length):
    rows = np.arange(length)[:, None]
    cols = np.arange(length)[None, :]
    half = length // 2
    frequency = np.where(cols <= half, cols, cols - half)
    phase = 2.0 * np.pi * (rows * frequency % length) / length
    table = np.where(cols <= half, np.cos(phase), np.sin(phase))
    edge = (cols == 0) | (cols == half)
    return (table * np.where(edge, np.sqrt(1.0 / length), np.sqrt(2.0 / length))).astype(np.float32)


def iota(shape, dim):
    return lax.broadcasted_iota(jnp.int32, shape, dim)


def eye(size):
    return (iota((size, size), 0) == iota((size, size), 1)).astype(jnp.float32)


def visits(members):
    return [(k * STRIDE) % members for k in range(1, members)]


def partner(me, offset):
    core = me % 2
    way = 1 + 2 * core
    x = ((me // 2) % 4 + way * ((offset // 2) % 4)) % 4
    z = ((me // 8) % 4 + way * ((offset // 8) % 4)) % 4
    y = (me // 32 + offset // 32) % 2
    return ((y * 4 + z) * 4 + x) * 2 + (core + offset % 2) % 2


def by_core(member, members):
    return (member % 2) * (members // 2) + member // 2


def thirds(a):
    first = a.astype(jnp.bfloat16)
    rest = a - first.astype(jnp.float32)
    second = rest.astype(jnp.bfloat16)
    return first, second, (rest - second.astype(jnp.float32)).astype(jnp.bfloat16)


def left_of(a):
    first, second, third = thirds(a)
    return jnp.concatenate([third, second, first, second, first, first], axis=1)


def product(a, b):
    first, second, third = thirds(b)
    right = jnp.concatenate([first, second, third, first, second, first], axis=0)
    return jnp.dot(left_of(a), right, preferred_element_type=jnp.float32)


def product_nt(a, b):
    first, second, third = thirds(b)
    right = jnp.concatenate([first, second, third, first, second, first], axis=1)
    return lax.dot_general(left_of(a), right, NT, preferred_element_type=jnp.float32)


def own_predictions(wall_ref, basis_t_ref, probe_ref, own_ref):
    planes, tile, modes = wall_ref.shape
    rows = planes * tile
    picked = iota((2 * planes, rows), 0)
    wanted = jnp.where(picked < planes, picked * tile + (tile - 1), (picked - planes) * tile + (tile - 2))
    pick = (iota((2 * planes, rows), 1) == wanted).astype(jnp.bfloat16)
    levels = jnp.dot(pick, wall_ref[...].reshape(rows, modes), preferred_element_type=jnp.float32)
    spectra_t = lax.dot_general(
        basis_t_ref[...], levels.astype(jnp.bfloat16), NT, preferred_element_type=jnp.float32
    ).astype(jnp.bfloat16)
    groups, width = own_ref.shape
    for g in range(groups):
        probe = probe_ref[:, g * width : (g + 1) * width]
        plane = ((probe >> 7) * 171) >> 9
        mode = probe - plane * modes
        row = iota((2 * planes, width), 0)
        sign = jnp.where(row == plane, 1.0, 0.0) - jnp.where(row == plane + planes, 1.0, 0.0)
        shear = jnp.dot(spectra_t, sign.astype(jnp.bfloat16), preferred_element_type=jnp.float32)
        taken = jnp.where(iota((modes, width), 0) == mode, shear, 0.0)
        own_ref[g : g + 1, :] = jnp.sum(taken, axis=0, keepdims=True)


def mixing_matrix(preds_ref, observed_ref, spread_ref, part_ref, block):
    cores, chips, groups, width = preds_ref.shape
    members = cores * chips
    side = 128
    inside = (iota((side, side), 0) < members) & (iota((side, side), 1) < members)
    unit = eye(side) * inside.astype(jnp.float32)
    gram = (members - 1.0) * unit
    right = jnp.zeros((1, side), jnp.float32)
    empty = jnp.zeros((side - members, width), jnp.float32)
    for g in range(groups):
        lanes = slice(g * width, (g + 1) * width)
        preds = preds_ref[:, :, g, :].reshape(members, width)
        mean = jnp.sum(preds, axis=0, keepdims=True) * (1.0 / members)
        selector = jnp.where(part_ref[:, lanes] == block, 1.0, 0.0) / spread_ref[:, lanes]
        scaled = jnp.concatenate([(preds - mean) * selector, empty], axis=0)
        innovation = (observed_ref[:, lanes] - mean) * selector
        gram += product_nt(scaled, scaled)
        right += product_nt(jnp.broadcast_to(innovation, (16, width)), scaled)[:1]
    squares = jnp.sum(jnp.sum(gram * gram, axis=1, keepdims=True), axis=0, keepdims=True)
    norm = jnp.sqrt(squares)

    def newton_iter(count, carry):
        iterate, inv_root = carry
        step = 1.5 * unit - 0.5 * product(inv_root, iterate)
        return product(iterate, step), product(step, inv_root)

    _, inv_root = lax.fori_loop(0, NS_ITERS, newton_iter, (gram / norm, unit))
    root = inv_root / jnp.sqrt(norm)
    inv_gram = product(root, root)
    factors = jnp.sum(inv_gram * right, axis=1, keepdims=True)
    combined = factors + np.float32(np.sqrt(members - 1.0)) * root
    combined = jnp.where(inside, combined, 0.0)
    centred = combined - jnp.sum(combined, axis=0, keepdims=True) * (1.0 / members)
    return jnp.where(inside, (1.0 / members) + centred - unit, 0.0).astype(jnp.bfloat16)


def kernel(
    members,
    x_ref,
    basis_hbm,
    basis_t_hbm,
    probe_hbm,
    part_hbm,
    observed_hbm,
    spread_hbm,
    weight_hbm,
    out_ref,
    basis_ref,
    basis_t_ref,
    probe_ref,
    part_ref,
    observed_ref,
    spread_ref,
    weight_ref,
    small_sem,
    wall,
    held,
    done,
    own,
    preds,
    spread_mix,
    spectra,
    wall_sem,
    give_sem,
    hold_sem,
    own_send,
    own_recv,
    preds_send,
    preds_recv,
    core_send,
    core_recv,
    back_send,
    back_recv,
):
    pieces, levels = held.shape[0], weight_ref.shape[0]
    deep = pieces * TILE // levels
    me = lax.axis_index("member")
    cell = lax.axis_index("cell")
    at_wall = cell == 1
    barrier = pltpu.get_barrier_semaphore()

    wall_copy = pltpu.make_async_copy(x_ref.at[0, :, pl.ds(levels - TILE, TILE)], wall, wall_sem)
    wall_copy.start()
    small = [
        pltpu.make_async_copy(source, target, small_sem.at[i])
        for i, (source, target) in enumerate(
            (
                (basis_t_hbm, basis_t_ref),
                (probe_hbm, probe_ref),
                (basis_hbm, basis_ref),
                (part_hbm, part_ref),
                (observed_hbm, observed_ref),
                (spread_hbm, spread_ref),
                (weight_hbm, weight_ref),
            )
        )
    ]
    for copy in small:
        copy.start()

    @pl.loop(1, members)
    def _(k):
        pl.semaphore_signal(barrier, inc=1, device_id={"member": (me + k) % members})

    pl.semaphore_signal(barrier, inc=1, device_id={"cell": 1 - cell})
    pl.semaphore_wait(barrier, members)

    def give(u):
        c, p = u // deep, u % deep
        rows = pl.ds(pl.multiple_of(c * TILE, TILE), TILE)
        pltpu.make_async_copy(x_ref.at[0, me * deep + p, rows], held.at[u, me], hold_sem.at[u]).start()
        for offset in visits(members):
            owner = partner(me, offset)
            pltpu.make_async_remote_copy(
                src_ref=x_ref.at[0, owner * deep + p, rows],
                dst_ref=held.at[u, me],
                send_sem=give_sem,
                recv_sem=hold_sem.at[u],
                device_id={"member": owner},
            ).start()

    @pl.loop(0, LEAD)
    def _(u):
        give(u)

    wall_copy.wait()
    small[0].wait()
    small[1].wait()
    to_sibling = pltpu.make_async_remote_copy(
        src_ref=own, dst_ref=own, send_sem=own_send, recv_sem=own_recv, device_id={"cell": 0}
    )

    @pl.when(at_wall)
    def _():
        own_predictions(wall, basis_t_ref, probe_ref, own)
        to_sibling.start()
        to_sibling.wait_send()

    @pl.when(jnp.logical_not(at_wall))
    def _():
        to_sibling.wait_recv()

    core, chip, chips = me % 2, me // 2, members // 2
    pltpu.make_async_copy(own, preds.at[core, chip], preds_recv).start()
    for offset in visits(members):
        if offset % 2 == 0:
            pltpu.make_async_remote_copy(
                src_ref=own,
                dst_ref=preds.at[core, chip],
                send_sem=preds_send,
                recv_sem=preds_recv,
                device_id={"member": partner(me, offset)},
            ).start()

    @pl.loop(LEAD, pieces)
    def _(u):
        give(u)

    for copy in small[2:]:
        copy.wait()
    pltpu.make_async_copy(preds.at[core], preds.at[core], preds_recv).wait()
    to_core = pltpu.make_async_remote_copy(
        src_ref=preds.at[core],
        dst_ref=preds.at[core],
        send_sem=core_send,
        recv_sem=core_recv,
        device_id={"member": me + 1 - 2 * core},
    )
    to_core.start()
    to_core.wait()
    mixing = mixing_matrix(preds, observed_ref, spread_ref, part_ref, me)

    wide = members * TILE
    high = 128
    across = (by_core(iota((high, wide), 1) // TILE, members) == iota((high, wide), 0)).astype(jnp.bfloat16)

    @pl.loop(0, wide // high)
    def _(b):
        member = (iota((high, high), 0) + b * high) // TILE
        down = (by_core(member, members) == iota((high, high), 1)).astype(jnp.bfloat16)
        part = lax.dot_general(down, mixing, NT, preferred_element_type=jnp.float32).astype(jnp.bfloat16)
        full = jnp.dot(part, across, preferred_element_type=jnp.float32)
        same = iota((high, wide), 0) % TILE == iota((high, wide), 1) % TILE
        spread_mix[pl.ds(pl.multiple_of(b * high, high), high), :] = jnp.where(same, full, 0.0).astype(jnp.bfloat16)

    step = 256
    some = step // TILE

    @pl.loop(0, pieces)
    def _(u):
        pltpu.make_async_copy(held.at[u], held.at[u], hold_sem.at[u]).wait()
        c, p = u // deep, u % deep
        rows = pl.ds(pl.multiple_of(c * TILE, TILE), TILE)

        @pl.loop(0, wide // step)
        def _(b):
            field = held[u, pl.ds(b * some, some)].reshape(step, -1)
            spectra[pl.ds(pl.multiple_of(b * step, step), step), :] = jnp.dot(
                field, basis_ref[...], preferred_element_type=jnp.float32
            ).astype(jnp.bfloat16)

        @pl.loop(0, wide // step)
        def _(b):
            changed = jnp.dot(
                spread_mix[pl.ds(pl.multiple_of(b * step, step), step), :],
                spectra[...],
                preferred_element_type=jnp.float32,
            )
            changed = changed.reshape(some, TILE, -1) * weight_ref[rows, :][None]
            changed = changed.astype(jnp.bfloat16).reshape(step, -1)
            back = jnp.dot(changed, basis_t_ref[...], preferred_element_type=jnp.float32)
            done[u, pl.ds(b * some, some)] = back.astype(jnp.bfloat16).reshape(some, TILE, -1)

        target = out_ref.at[0, me * deep + p, rows]
        pltpu.make_async_copy(done.at[u, me], target, back_recv).start()
        for offset in visits(members):
            member = partner(me, offset)
            pltpu.make_async_remote_copy(
                src_ref=done.at[u, member],
                dst_ref=target,
                send_sem=back_send,
                recv_sem=back_recv,
                device_id={"member": member},
            ).start()

    others = pl.ds(0, members - 1)
    far = preds.at[0, pl.ds(0, chips - 1)]
    pltpu.make_async_copy(far, far, preds_send).wait()
    pltpu.make_async_copy(held.at[:, others], held.at[:, others], give_sem).wait()
    pltpu.make_async_copy(held.at[:, others], held.at[:, others], back_send).wait()
    pltpu.make_async_copy(out_ref, out_ref, back_recv).wait()


def copy_out(source, target, buffer, come, go):
    parts = buffer.shape[0]
    deep = buffer.shape[2]
    reads, writes = [], []
    for i in range(parts):
        planes = pl.ds(i * deep, deep)
        reads.append(pltpu.make_async_copy(source.at[:, planes], buffer.at[i], come.at[i]))
        writes.append(pltpu.make_async_copy(buffer.at[i], target.at[:, planes], go.at[i]))
        reads[-1].start()
    for i in range(parts):
        reads[i].wait()
        writes[i].start()
    for i in range(parts):
        writes[i].wait()


def on_device(members, x, probe, part, observed, spread, weight):
    _, planes, levels, modes = x.shape
    sensors = probe.shape[0]
    pieces = (levels // TILE) * (planes // members)
    table = dft_basis(modes)
    basis = jnp.asarray(table, jnp.bfloat16)
    basis_t = jnp.asarray(table.T, jnp.bfloat16)
    hbm = pl.BlockSpec(memory_space=pltpu.HBM)
    dma = pltpu.SemaphoreType.DMA(())
    increments = pl.pallas_call(
        functools.partial(kernel, members),
        out_shape=jax.ShapeDtypeStruct(x.shape, x.dtype),
        in_specs=[hbm] * 8,
        out_specs=hbm,
        scratch_shapes=[
            pltpu.VMEM((modes, modes), jnp.bfloat16),
            pltpu.VMEM((modes, modes), jnp.bfloat16),
            pltpu.VMEM((1, sensors), jnp.int32),
            pltpu.VMEM((1, sensors), jnp.int32),
            pltpu.VMEM((1, sensors), jnp.float32),
            pltpu.VMEM((1, sensors), jnp.float32),
            pltpu.VMEM((levels, modes), jnp.float32),
            pltpu.SemaphoreType.DMA((7,)),
            pltpu.VMEM((planes, TILE, modes), jnp.bfloat16),
            pltpu.VMEM((pieces, members, TILE, modes), jnp.bfloat16),
            pltpu.VMEM((pieces, members, TILE, modes), jnp.bfloat16),
            pltpu.VMEM((8, sensors // 8), jnp.float32),
            pltpu.VMEM((2, members // 2, 8, sensors // 8), jnp.float32),
            pltpu.VMEM((members * TILE, members * TILE), jnp.bfloat16),
            pltpu.VMEM((members * TILE, modes), jnp.bfloat16),
            dma,
            dma,
            pltpu.SemaphoreType.DMA((pieces,)),
            dma,
            dma,
            dma,
            dma,
            dma,
            dma,
            dma,
            dma,
        ],
        compiler_params=pltpu.CompilerParams(
            collective_id=0, has_side_effects=True, vmem_limit_bytes=60 << 20
        ),
    )(x, basis, basis_t, probe[None], part[None], observed[None], spread[None], weight)
    parts = 8
    return pl.pallas_call(
        copy_out,
        out_shape=jax.ShapeDtypeStruct(x.shape, x.dtype),
        in_specs=[hbm],
        out_specs=hbm,
        scratch_shapes=[
            pltpu.VMEM((parts, 1, planes // parts, levels, modes), x.dtype),
            pltpu.SemaphoreType.DMA((parts,)),
            pltpu.SemaphoreType.DMA((parts,)),
        ],
        compiler_params=pltpu.CompilerParams(vmem_limit_bytes=60 << 20),
    )(increments)


def solution(mesh):
    return jax.shard_map(
        functools.partial(on_device, mesh.shape["member"]),
        mesh=mesh,
        in_specs=(P("member", None, "cell", None), P(), P(), P(), P(), P("cell", None)),
        out_specs=P("member", None, "cell", None),
        check_vma=False,
    )
```

```python
import functools

import jax
import jax.numpy as jnp
import numpy as np
from jax import lax
from jax.experimental import pallas as pl
from jax.experimental.pallas import tpu as pltpu
from jax.sharding import PartitionSpec as P

NS_ITERS = 24
STRIDE = 37
TILE = 16
LEAD = 3
NT = (((1,), (1,)), ((), ()))


def dft_basis(length):
    rows = np.arange(length)[:, None]
    cols = np.arange(length)[None, :]
    half = length // 2
    frequency = np.where(cols <= half, cols, cols - half)
    phase = 2.0 * np.pi * (rows * frequency % length) / length
    table = np.where(cols <= half, np.cos(phase), np.sin(phase))
    edge = (cols == 0) | (cols == half)
    return (table * np.where(edge, np.sqrt(1.0 / length), np.sqrt(2.0 / length))).astype(np.float32)


def iota(shape, dim):
    return lax.broadcasted_iota(jnp.int32, shape, dim)


def eye(size):
    return (iota((size, size), 0) == iota((size, size), 1)).astype(jnp.float32)


def visits(members):
    return [(k * STRIDE) % members for k in range(1, members)]


def partner(me, offset):
    core = me % 2
    way = 1 + 2 * core
    x = ((me // 2) % 4 + way * ((offset // 2) % 4)) % 4
    z = ((me // 8) % 4 + way * ((offset // 8) % 4)) % 4
    y = (me // 32 + offset // 32) % 2
    return ((y * 4 + z) * 4 + x) * 2 + (core + offset % 2) % 2


def by_core(member, members):
    return (member % 2) * (members // 2) + member // 2


def thirds(a):
    first = a.astype(jnp.bfloat16)
    rest = a - first.astype(jnp.float32)
    second = rest.astype(jnp.bfloat16)
    return first, second, (rest - second.astype(jnp.float32)).astype(jnp.bfloat16)


def left_of(a):
    first, second, third = thirds(a)
    return jnp.concatenate([third, second, first, second, first, first], axis=1)


def product(a, b):
    first, second, third = thirds(b)
    right = jnp.concatenate([first, second, third, first, second, first], axis=0)
    return jnp.dot(left_of(a), right, preferred_element_type=jnp.float32)


def product_nt(a, b):
    first, second, third = thirds(b)
    right = jnp.concatenate([first, second, third, first, second, first], axis=1)
    return lax.dot_general(left_of(a), right, NT, preferred_element_type=jnp.float32)


def own_predictions(wall_ref, basis_t_ref, probe_ref, own_ref):
    planes, tile, modes = wall_ref.shape
    rows = planes * tile
    picked = iota((2 * planes, rows), 0)
    wanted = jnp.where(picked < planes, picked * tile + (tile - 1), (picked - planes) * tile + (tile - 2))
    pick = (iota((2 * planes, rows), 1) == wanted).astype(jnp.bfloat16)
    levels = jnp.dot(pick, wall_ref[...].reshape(rows, modes), preferred_element_type=jnp.float32)
    spectra_t = lax.dot_general(
        basis_t_ref[...], levels.astype(jnp.bfloat16), NT, preferred_element_type=jnp.float32
    ).astype(jnp.bfloat16)
    groups, width = own_ref.shape
    for g in range(groups):
        probe = probe_ref[:, g * width : (g + 1) * width]
        plane = ((probe >> 7) * 171) >> 9
        mode = probe - plane * modes
        row = iota((2 * planes, width), 0)
        sign = jnp.where(row == plane, 1.0, 0.0) - jnp.where(row == plane + planes, 1.0, 0.0)
        shear = jnp.dot(spectra_t, sign.astype(jnp.bfloat16), preferred_element_type=jnp.float32)
        taken = jnp.where(iota((modes, width), 0) == mode, shear, 0.0)
        own_ref[g : g + 1, :] = jnp.sum(taken, axis=0, keepdims=True)


def mixing_matrix(preds_ref, observed_ref, spread_ref, part_ref, block):
    cores, chips, groups, width = preds_ref.shape
    members = cores * chips
    side = 128
    inside = (iota((side, side), 0) < members) & (iota((side, side), 1) < members)
    unit = eye(side) * inside.astype(jnp.float32)
    gram = (members - 1.0) * unit
    right = jnp.zeros((1, side), jnp.float32)
    empty = jnp.zeros((side - members, width), jnp.float32)
    for g in range(groups):
        lanes = slice(g * width, (g + 1) * width)
        preds = preds_ref[:, :, g, :].reshape(members, width)
        mean = jnp.sum(preds, axis=0, keepdims=True) * (1.0 / members)
        selector = jnp.where(part_ref[:, lanes] == block, 1.0, 0.0) / spread_ref[:, lanes]
        scaled = jnp.concatenate([(preds - mean) * selector, empty], axis=0)
        innovation = (observed_ref[:, lanes] - mean) * selector
        gram += product_nt(scaled, scaled)
        right += product_nt(jnp.broadcast_to(innovation, (16, width)), scaled)[:1]
    squares = jnp.sum(jnp.sum(gram * gram, axis=1, keepdims=True), axis=0, keepdims=True)
    norm = jnp.sqrt(squares)

    def newton_iter(count, carry):
        iterate, inv_root = carry
        step = 1.5 * unit - 0.5 * product(inv_root, iterate)
        return product(iterate, step), product(step, inv_root)

    _, inv_root = lax.fori_loop(0, NS_ITERS, newton_iter, (gram / norm, unit))
    root = inv_root / jnp.sqrt(norm)
    inv_gram = product(root, root)
    factors = jnp.sum(inv_gram * right, axis=1, keepdims=True)
    combined = factors + np.float32(np.sqrt(members - 1.0)) * root
    combined = jnp.where(inside, combined, 0.0)
    centred = combined - jnp.sum(combined, axis=0, keepdims=True) * (1.0 / members)
    return jnp.where(inside, (1.0 / members) + centred - unit, 0.0).astype(jnp.bfloat16)


def kernel(
    members,
    x_ref,
    basis_hbm,
    basis_t_hbm,
    probe_hbm,
    part_hbm,
    observed_hbm,
    spread_hbm,
    weight_hbm,
    out_ref,
    basis_ref,
    basis_t_ref,
    probe_ref,
    part_ref,
    observed_ref,
    spread_ref,
    weight_ref,
    small_sem,
    wall,
    held,
    done,
    own,
    preds,
    spread_mix,
    spectra,
    wall_sem,
    give_sem,
    hold_sem,
    own_send,
    own_recv,
    preds_send,
    preds_recv,
    core_send,
    core_recv,
    back_send,
    back_recv,
):
    pieces, levels = held.shape[0], weight_ref.shape[0]
    deep = pieces * TILE // levels
    me = lax.axis_index("member")
    cell = lax.axis_index("cell")
    at_wall = cell == 1
    barrier = pltpu.get_barrier_semaphore()

    wall_copy = pltpu.make_async_copy(x_ref.at[0, :, pl.ds(levels - TILE, TILE)], wall, wall_sem)
    wall_copy.start()
    small = [
        pltpu.make_async_copy(source, target, small_sem.at[i])
        for i, (source, target) in enumerate(
            (
                (basis_t_hbm, basis_t_ref),
                (probe_hbm, probe_ref),
                (basis_hbm, basis_ref),
                (part_hbm, part_ref),
                (observed_hbm, observed_ref),
                (spread_hbm, spread_ref),
                (weight_hbm, weight_ref),
            )
        )
    ]
    for copy in small:
        copy.start()

    @pl.loop(1, members)
    def _(k):
        pl.semaphore_signal(barrier, inc=1, device_id={"member": (me + k) % members})

    pl.semaphore_signal(barrier, inc=1, device_id={"cell": 1 - cell})
    pl.semaphore_wait(barrier, members)

    def give(u):
        c, p = u // deep, u % deep
        rows = pl.ds(pl.multiple_of(c * TILE, TILE), TILE)
        pltpu.make_async_copy(x_ref.at[0, me * deep + p, rows], held.at[u, me], hold_sem.at[u]).start()
        for offset in visits(members):
            owner = partner(me, offset)
            pltpu.make_async_remote_copy(
                src_ref=x_ref.at[0, owner * deep + p, rows],
                dst_ref=held.at[u, me],
                send_sem=give_sem,
                recv_sem=hold_sem.at[u],
                device_id={"member": owner},
            ).start()

    @pl.loop(0, LEAD)
    def _(u):
        give(u)

    wall_copy.wait()
    small[0].wait()
    small[1].wait()
    to_sibling = pltpu.make_async_remote_copy(
        src_ref=own, dst_ref=own, send_sem=own_send, recv_sem=own_recv, device_id={"cell": 0}
    )

    @pl.when(at_wall)
    def _():
        own_predictions(wall, basis_t_ref, probe_ref, own)
        to_sibling.start()
        to_sibling.wait_send()

    @pl.when(jnp.logical_not(at_wall))
    def _():
        to_sibling.wait_recv()

    core, chip, chips = me % 2, me // 2, members // 2
    pltpu.make_async_copy(own, preds.at[core, chip], preds_recv).start()
    for offset in visits(members):
        if offset % 2 == 0:
            pltpu.make_async_remote_copy(
                src_ref=own,
                dst_ref=preds.at[core, chip],
                send_sem=preds_send,
                recv_sem=preds_recv,
                device_id={"member": partner(me, offset)},
            ).start()

    @pl.loop(LEAD, pieces)
    def _(u):
        give(u)

    for copy in small[2:]:
        copy.wait()
    pltpu.make_async_copy(preds.at[core], preds.at[core], preds_recv).wait()
    to_core = pltpu.make_async_remote_copy(
        src_ref=preds.at[core],
        dst_ref=preds.at[core],
        send_sem=core_send,
        recv_sem=core_recv,
        device_id={"member": me + 1 - 2 * core},
    )
    to_core.start()
    to_core.wait()
    mixing = mixing_matrix(preds, observed_ref, spread_ref, part_ref, me)

    wide = members * TILE
    high = 128
    across = (by_core(iota((high, wide), 1) // TILE, members) == iota((high, wide), 0)).astype(jnp.bfloat16)

    @pl.loop(0, wide // high)
    def _(b):
        member = (iota((high, high), 0) + b * high) // TILE
        down = (by_core(member, members) == iota((high, high), 1)).astype(jnp.bfloat16)
        part = lax.dot_general(down, mixing, NT, preferred_element_type=jnp.float32).astype(jnp.bfloat16)
        full = jnp.dot(part, across, preferred_element_type=jnp.float32)
        same = iota((high, wide), 0) % TILE == iota((high, wide), 1) % TILE
        spread_mix[pl.ds(pl.multiple_of(b * high, high), high), :] = jnp.where(same, full, 0.0).astype(jnp.bfloat16)

    step = 256
    some = step // TILE

    @pl.loop(0, pieces)
    def _(u):
        pltpu.make_async_copy(held.at[u], held.at[u], hold_sem.at[u]).wait()
        c, p = u // deep, u % deep
        rows = pl.ds(pl.multiple_of(c * TILE, TILE), TILE)

        @pl.loop(0, wide // step)
        def _(b):
            field = held[u, pl.ds(b * some, some)].reshape(step, -1)
            spectra[pl.ds(pl.multiple_of(b * step, step), step), :] = jnp.dot(
                field, basis_ref[...], preferred_element_type=jnp.float32
            ).astype(jnp.bfloat16)

        @pl.loop(0, wide // step)
        def _(b):
            changed = jnp.dot(
                spread_mix[pl.ds(pl.multiple_of(b * step, step), step), :],
                spectra[...],
                preferred_element_type=jnp.float32,
            )
            changed = changed.reshape(some, TILE, -1) * weight_ref[rows, :][None]
            changed = changed.astype(jnp.bfloat16).reshape(step, -1)
            back = jnp.dot(changed, basis_t_ref[...], preferred_element_type=jnp.float32)
            done[u, pl.ds(b * some, some)] = back.astype(jnp.bfloat16).reshape(some, TILE, -1)

        target = out_ref.at[0, me * deep + p, rows]
        pltpu.make_async_copy(done.at[u, me], target, back_recv).start()
        for offset in visits(members):
            member = partner(me, offset)
            pltpu.make_async_remote_copy(
                src_ref=done.at[u, member],
                dst_ref=target,
                send_sem=back_send,
                recv_sem=back_recv,
                device_id={"member": member},
            ).start()

    others = pl.ds(0, members - 1)
    far = preds.at[0, pl.ds(0, chips - 1)]
    pltpu.make_async_copy(far, far, preds_send).wait()
    pltpu.make_async_copy(held.at[:, others], held.at[:, others], give_sem).wait()
    pltpu.make_async_copy(held.at[:, others], held.at[:, others], back_send).wait()
    pltpu.make_async_copy(out_ref, out_ref, back_recv).wait()


def copy_out(source, target, go):
    parts = go.shape[0]
    deep = source.shape[1] // parts
    writes = []
    for i in range(parts):
        planes = pl.ds(i * deep, deep)
        writes.append(pltpu.make_async_copy(source.at[:, planes], target.at[:, planes], go.at[i]))
        writes[-1].start()
    for write in writes:
        write.wait()


def on_device(members, x, probe, part, observed, spread, weight):
    _, planes, levels, modes = x.shape
    sensors = probe.shape[0]
    pieces = (levels // TILE) * (planes // members)
    table = dft_basis(modes)
    basis = jnp.asarray(table, jnp.bfloat16)
    basis_t = jnp.asarray(table.T, jnp.bfloat16)
    vmem = pl.BlockSpec(memory_space=pltpu.VMEM)
    hbm = pl.BlockSpec(memory_space=pltpu.HBM)
    dma = pltpu.SemaphoreType.DMA(())
    increments = pl.pallas_call(
        functools.partial(kernel, members),
        out_shape=jax.ShapeDtypeStruct(x.shape, x.dtype),
        in_specs=[hbm] * 8,
        out_specs=vmem,
        scratch_shapes=[
            pltpu.VMEM((modes, modes), jnp.bfloat16),
            pltpu.VMEM((modes, modes), jnp.bfloat16),
            pltpu.VMEM((1, sensors), jnp.int32),
            pltpu.VMEM((1, sensors), jnp.int32),
            pltpu.VMEM((1, sensors), jnp.float32),
            pltpu.VMEM((1, sensors), jnp.float32),
            pltpu.VMEM((levels, modes), jnp.float32),
            pltpu.SemaphoreType.DMA((7,)),
            pltpu.VMEM((planes, TILE, modes), jnp.bfloat16),
            pltpu.VMEM((pieces, members, TILE, modes), jnp.bfloat16),
            pltpu.VMEM((pieces, members, TILE, modes), jnp.bfloat16),
            pltpu.VMEM((8, sensors // 8), jnp.float32),
            pltpu.VMEM((2, members // 2, 8, sensors // 8), jnp.float32),
            pltpu.VMEM((members * TILE, members * TILE), jnp.bfloat16),
            pltpu.VMEM((members * TILE, modes), jnp.bfloat16),
            dma,
            dma,
            pltpu.SemaphoreType.DMA((pieces,)),
            dma,
            dma,
            dma,
            dma,
            dma,
            dma,
            dma,
            dma,
        ],
        compiler_params=pltpu.CompilerParams(
            collective_id=0, has_side_effects=True, vmem_limit_bytes=37748736
        ),
    )(x, *(pltpu.with_memory_space_constraint(a, pltpu.HBM) for a in (basis, basis_t, probe[None], part[None], observed[None], spread[None], weight)))
    parts = 8
    return pl.pallas_call(
        copy_out,
        out_shape=jax.ShapeDtypeStruct(x.shape, x.dtype),
        in_specs=[vmem],
        out_specs=hbm,
        scratch_shapes=[
            pltpu.SemaphoreType.DMA((parts,)),
        ],
        compiler_params=pltpu.CompilerParams(vmem_limit_bytes=1 << 20),
    )(increments)


def solution(mesh):
    return jax.shard_map(
        functools.partial(on_device, mesh.shape["member"]),
        mesh=mesh,
        in_specs=(P("member", None, "cell", None), P(), P(), P(), P(), P("cell", None)),
        out_specs=P("member", None, "cell", None),
        check_vma=False,
    )
```

```python
import functools

import jax
import jax.numpy as jnp
import numpy as np
from jax import lax
from jax.experimental import pallas as pl
from jax.experimental.pallas import tpu as pltpu
from jax.sharding import PartitionSpec as P

NS_ITERS = 24
STRIDE = 37
TILE = 16
LAST = 2
LEAD = 3
NT = (((1,), (1,)), ((), ()))


def dft_basis(length):
    rows = np.arange(length)[:, None]
    cols = np.arange(length)[None, :]
    half = length // 2
    frequency = np.where(cols <= half, cols, cols - half)
    phase = 2.0 * np.pi * (rows * frequency % length) / length
    table = np.where(cols <= half, np.cos(phase), np.sin(phase))
    edge = (cols == 0) | (cols == half)
    return (table * np.where(edge, np.sqrt(1.0 / length), np.sqrt(2.0 / length))).astype(np.float32)


def iota(shape, dim):
    return lax.broadcasted_iota(jnp.int32, shape, dim)


def eye(size):
    return (iota((size, size), 0) == iota((size, size), 1)).astype(jnp.float32)


def visits(members):
    return [(k * STRIDE) % members for k in range(1, members)]


def hops(offset):
    across = [0, 1, 2, 1]
    return across[(offset // 2) % 4] + across[(offset // 8) % 4] + 2 * (offset // 32)


def partner(me, offset):
    core = me % 2
    way = 1 + 2 * core
    x = ((me // 2) % 4 + way * ((offset // 2) % 4)) % 4
    z = ((me // 8) % 4 + way * ((offset // 8) % 4)) % 4
    y = (me // 32 + offset // 32) % 2
    return ((y * 4 + z) * 4 + x) * 2 + (core + offset % 2) % 2


def by_core(member, members):
    return (member % 2) * (members // 2) + member // 2


def thirds(a):
    first = a.astype(jnp.bfloat16)
    rest = a - first.astype(jnp.float32)
    second = rest.astype(jnp.bfloat16)
    return first, second, (rest - second.astype(jnp.float32)).astype(jnp.bfloat16)


def left_of(a):
    first, second, third = thirds(a)
    return jnp.concatenate([third, second, first, second, first, first], axis=1)


def product(a, b):
    first, second, third = thirds(b)
    right = jnp.concatenate([first, second, third, first, second, first], axis=0)
    return jnp.dot(left_of(a), right, preferred_element_type=jnp.float32)


def product_nt(a, b):
    first, second, third = thirds(b)
    right = jnp.concatenate([first, second, third, first, second, first], axis=1)
    return lax.dot_general(left_of(a), right, NT, preferred_element_type=jnp.float32)


def own_predictions(wall_ref, basis_t_ref, probe_ref, own_ref):
    planes, tile, modes = wall_ref.shape
    rows = planes * tile
    picked = iota((2 * planes, rows), 0)
    wanted = jnp.where(picked < planes, picked * tile + (tile - 1), (picked - planes) * tile + (tile - 2))
    pick = (iota((2 * planes, rows), 1) == wanted).astype(jnp.bfloat16)
    levels = jnp.dot(pick, wall_ref[...].reshape(rows, modes), preferred_element_type=jnp.float32)
    spectra_t = lax.dot_general(
        basis_t_ref[...], levels.astype(jnp.bfloat16), NT, preferred_element_type=jnp.float32
    ).astype(jnp.bfloat16)
    groups, width = own_ref.shape
    for g in range(groups):
        probe = probe_ref[:, g * width : (g + 1) * width]
        plane = ((probe >> 7) * 171) >> 9
        mode = probe - plane * modes
        row = iota((2 * planes, width), 0)
        sign = jnp.where(row == plane, 1.0, 0.0) - jnp.where(row == plane + planes, 1.0, 0.0)
        shear = jnp.dot(spectra_t, sign.astype(jnp.bfloat16), preferred_element_type=jnp.float32)
        taken = jnp.where(iota((modes, width), 0) == mode, shear, 0.0)
        own_ref[g : g + 1, :] = jnp.sum(taken, axis=0, keepdims=True)


def mixing_matrix(preds_ref, observed_ref, spread_ref, part_ref, block):
    cores, chips, groups, width = preds_ref.shape
    members = cores * chips
    side = 128
    inside = (iota((side, side), 0) < members) & (iota((side, side), 1) < members)
    unit = eye(side) * inside.astype(jnp.float32)
    gram = (members - 1.0) * unit
    right = jnp.zeros((1, side), jnp.float32)
    empty = jnp.zeros((side - members, width), jnp.float32)
    for g in range(groups):
        lanes = slice(g * width, (g + 1) * width)
        preds = preds_ref[:, :, g, :].reshape(members, width)
        mean = jnp.sum(preds, axis=0, keepdims=True) * (1.0 / members)
        selector = jnp.where(part_ref[:, lanes] == block, 1.0, 0.0) / spread_ref[:, lanes]
        scaled = jnp.concatenate([(preds - mean) * selector, empty], axis=0)
        innovation = (observed_ref[:, lanes] - mean) * selector
        gram += product_nt(scaled, scaled)
        right += product_nt(jnp.broadcast_to(innovation, (16, width)), scaled)[:1]
    squares = jnp.sum(jnp.sum(gram * gram, axis=1, keepdims=True), axis=0, keepdims=True)
    norm = jnp.sqrt(squares)

    def newton_iter(count, carry):
        iterate, inv_root = carry
        step = 1.5 * unit - 0.5 * product(inv_root, iterate)
        return product(iterate, step), product(step, inv_root)

    _, inv_root = lax.fori_loop(0, NS_ITERS, newton_iter, (gram / norm, unit))
    root = inv_root / jnp.sqrt(norm)
    inv_gram = product(root, root)
    factors = jnp.sum(inv_gram * right, axis=1, keepdims=True)
    combined = factors + np.float32(np.sqrt(members - 1.0)) * root
    combined = jnp.where(inside, combined, 0.0)
    centred = combined - jnp.sum(combined, axis=0, keepdims=True) * (1.0 / members)
    return jnp.where(inside, (1.0 / members) + centred - unit, 0.0).astype(jnp.bfloat16)


def kernel(
    members,
    x_ref,
    basis_hbm,
    basis_t_hbm,
    probe_hbm,
    part_hbm,
    observed_hbm,
    spread_hbm,
    weight_hbm,
    out_ref,
    basis_ref,
    basis_t_ref,
    probe_ref,
    part_ref,
    observed_ref,
    spread_ref,
    weight_ref,
    small_sem,
    wall,
    held,
    done,
    own,
    preds,
    spread_mix,
    spectra,
    wall_sem,
    give_sem,
    hold_sem,
    own_send,
    own_recv,
    preds_send,
    preds_recv,
    core_send,
    core_recv,
    back_send,
    back_recv,
):
    pieces, levels = held.shape[0], weight_ref.shape[0]
    deep = pieces * TILE // levels
    me = lax.axis_index("member")
    cell = lax.axis_index("cell")
    at_wall = cell == 1
    barrier = pltpu.get_barrier_semaphore()

    wall_copy = pltpu.make_async_copy(x_ref.at[0, :, pl.ds(levels - TILE, TILE)], wall, wall_sem)
    wall_copy.start()
    small = [
        pltpu.make_async_copy(source, target, small_sem.at[i])
        for i, (source, target) in enumerate(
            (
                (basis_t_hbm, basis_t_ref),
                (probe_hbm, probe_ref),
                (basis_hbm, basis_ref),
                (part_hbm, part_ref),
                (observed_hbm, observed_ref),
                (spread_hbm, spread_ref),
                (weight_hbm, weight_ref),
            )
        )
    ]
    for copy in small:
        copy.start()

    @pl.loop(1, members)
    def _(k):
        pl.semaphore_signal(barrier, inc=1, device_id={"member": (me + k) % members})

    pl.semaphore_signal(barrier, inc=1, device_id={"cell": 1 - cell})
    pl.semaphore_wait(barrier, members)

    def give(u):
        c, p = u // deep, u % deep
        rows = pl.ds(pl.multiple_of(c * TILE, TILE), TILE)
        pltpu.make_async_copy(x_ref.at[0, me * deep + p, rows], held.at[u, me], hold_sem.at[u]).start()
        for offset in visits(members):
            owner = partner(me, offset)
            pltpu.make_async_remote_copy(
                src_ref=x_ref.at[0, owner * deep + p, rows],
                dst_ref=held.at[u, me],
                send_sem=give_sem,
                recv_sem=hold_sem.at[u],
                device_id={"member": owner},
            ).start()

    @pl.loop(0, LEAD)
    def _(u):
        give(u)

    wall_copy.wait()
    small[0].wait()
    small[1].wait()
    to_sibling = pltpu.make_async_remote_copy(
        src_ref=own, dst_ref=own, send_sem=own_send, recv_sem=own_recv, device_id={"cell": 0}
    )

    @pl.when(at_wall)
    def _():
        own_predictions(wall, basis_t_ref, probe_ref, own)
        to_sibling.start()
        to_sibling.wait_send()

    @pl.when(jnp.logical_not(at_wall))
    def _():
        to_sibling.wait_recv()

    core, chip, chips = me % 2, me // 2, members // 2
    pltpu.make_async_copy(own, preds.at[core, chip], preds_recv).start()
    for offset in visits(members):
        if offset % 2 == 0:
            pltpu.make_async_remote_copy(
                src_ref=own,
                dst_ref=preds.at[core, chip],
                send_sem=preds_send,
                recv_sem=preds_recv,
                device_id={"member": partner(me, offset)},
            ).start()

    @pl.loop(LEAD, pieces)
    def _(u):
        give(u)

    for copy in small[2:]:
        copy.wait()
    pltpu.make_async_copy(preds.at[core], preds.at[core], preds_recv).wait()
    to_core = pltpu.make_async_remote_copy(
        src_ref=preds.at[core],
        dst_ref=preds.at[core],
        send_sem=core_send,
        recv_sem=core_recv,
        device_id={"member": me + 1 - 2 * core},
    )
    to_core.start()
    to_core.wait()
    mixing = mixing_matrix(preds, observed_ref, spread_ref, part_ref, me)

    wide = members * TILE
    high = 128
    across = (by_core(iota((high, wide), 1) // TILE, members) == iota((high, wide), 0)).astype(jnp.bfloat16)

    @pl.loop(0, wide // high)
    def _(b):
        member = (iota((high, high), 0) + b * high) // TILE
        down = (by_core(member, members) == iota((high, high), 1)).astype(jnp.bfloat16)
        part = lax.dot_general(down, mixing, NT, preferred_element_type=jnp.float32).astype(jnp.bfloat16)
        full = jnp.dot(part, across, preferred_element_type=jnp.float32)
        same = iota((high, wide), 0) % TILE == iota((high, wide), 1) % TILE
        spread_mix[pl.ds(pl.multiple_of(b * high, high), high), :] = jnp.where(same, full, 0.0).astype(jnp.bfloat16)

    step = 256
    some = step // TILE

    @pl.loop(0, pieces)
    def _(u):
        pltpu.make_async_copy(held.at[u], held.at[u], hold_sem.at[u]).wait()
        c, p = u // deep, u % deep
        rows = pl.ds(pl.multiple_of(c * TILE, TILE), TILE)

        @pl.loop(0, wide // step)
        def _(b):
            field = held[u, pl.ds(b * some, some)].reshape(step, -1)
            spectra[pl.ds(pl.multiple_of(b * step, step), step), :] = jnp.dot(
                field, basis_ref[...], preferred_element_type=jnp.float32
            ).astype(jnp.bfloat16)

        @pl.loop(0, wide // step)
        def _(b):
            changed = jnp.dot(
                spread_mix[pl.ds(pl.multiple_of(b * step, step), step), :],
                spectra[...],
                preferred_element_type=jnp.float32,
            )
            changed = changed.reshape(some, TILE, -1) * weight_ref[rows, :][None]
            changed = changed.astype(jnp.bfloat16).reshape(step, -1)
            back = jnp.dot(changed, basis_t_ref[...], preferred_element_type=jnp.float32)
            done[u, pl.ds(b * some, some)] = back.astype(jnp.bfloat16).reshape(some, TILE, -1)

        target = out_ref.at[0, me * deep + p, rows]
        pltpu.make_async_copy(done.at[u, me], target, back_recv).start()

        def give_back(order):
            for offset in order:
                member = partner(me, offset)
                pltpu.make_async_remote_copy(
                    src_ref=done.at[u, member],
                    dst_ref=target,
                    send_sem=back_send,
                    recv_sem=back_recv,
                    device_id={"member": member},
                ).start()

        @pl.when(u < pieces - LAST)
        def _():
            give_back(visits(members))

        @pl.when(u >= pieces - LAST)
        def _():
            give_back(sorted(visits(members), key=lambda offset: -hops(offset)))

    others = pl.ds(0, members - 1)
    far = preds.at[0, pl.ds(0, chips - 1)]
    pltpu.make_async_copy(far, far, preds_send).wait()
    pltpu.make_async_copy(held.at[:, others], held.at[:, others], give_sem).wait()
    pltpu.make_async_copy(held.at[:, others], held.at[:, others], back_send).wait()
    pltpu.make_async_copy(out_ref, out_ref, back_recv).wait()


def copy_out(source, target, go):
    parts = go.shape[0]
    deep = source.shape[1] // parts
    writes = []
    for i in range(parts):
        planes = pl.ds(i * deep, deep)
        writes.append(pltpu.make_async_copy(source.at[:, planes], target.at[:, planes], go.at[i]))
        writes[-1].start()
    for write in writes:
        write.wait()


def on_device(members, x, probe, part, observed, spread, weight):
    _, planes, levels, modes = x.shape
    sensors = probe.shape[0]
    pieces = (levels // TILE) * (planes // members)
    table = dft_basis(modes)
    basis = jnp.asarray(table, jnp.bfloat16)
    basis_t = jnp.asarray(table.T, jnp.bfloat16)
    vmem = pl.BlockSpec(memory_space=pltpu.VMEM)
    hbm = pl.BlockSpec(memory_space=pltpu.HBM)
    dma = pltpu.SemaphoreType.DMA(())
    increments = pl.pallas_call(
        functools.partial(kernel, members),
        out_shape=jax.ShapeDtypeStruct(x.shape, x.dtype),
        in_specs=[hbm] * 8,
        out_specs=vmem,
        scratch_shapes=[
            pltpu.VMEM((modes, modes), jnp.bfloat16),
            pltpu.VMEM((modes, modes), jnp.bfloat16),
            pltpu.VMEM((1, sensors), jnp.int32),
            pltpu.VMEM((1, sensors), jnp.int32),
            pltpu.VMEM((1, sensors), jnp.float32),
            pltpu.VMEM((1, sensors), jnp.float32),
            pltpu.VMEM((levels, modes), jnp.float32),
            pltpu.SemaphoreType.DMA((7,)),
            pltpu.VMEM((planes, TILE, modes), jnp.bfloat16),
            pltpu.VMEM((pieces, members, TILE, modes), jnp.bfloat16),
            pltpu.VMEM((pieces, members, TILE, modes), jnp.bfloat16),
            pltpu.VMEM((8, sensors // 8), jnp.float32),
            pltpu.VMEM((2, members // 2, 8, sensors // 8), jnp.float32),
            pltpu.VMEM((members * TILE, members * TILE), jnp.bfloat16),
            pltpu.VMEM((members * TILE, modes), jnp.bfloat16),
            dma,
            dma,
            pltpu.SemaphoreType.DMA((pieces,)),
            dma,
            dma,
            dma,
            dma,
            dma,
            dma,
            dma,
            dma,
        ],
        compiler_params=pltpu.CompilerParams(
            collective_id=0, has_side_effects=True, vmem_limit_bytes=37748736
        ),
    )(x, *(pltpu.with_memory_space_constraint(a, pltpu.HBM) for a in (basis, basis_t, probe[None], part[None], observed[None], spread[None], weight)))
    parts = 8
    return pl.pallas_call(
        copy_out,
        out_shape=jax.ShapeDtypeStruct(x.shape, x.dtype),
        in_specs=[vmem],
        out_specs=hbm,
        scratch_shapes=[
            pltpu.SemaphoreType.DMA((parts,)),
        ],
        compiler_params=pltpu.CompilerParams(vmem_limit_bytes=1 << 20),
    )(increments)


def solution(mesh):
    return jax.shard_map(
        functools.partial(on_device, mesh.shape["member"]),
        mesh=mesh,
        in_specs=(P("member", None, "cell", None), P(), P(), P(), P(), P("cell", None)),
        out_specs=P("member", None, "cell", None),
        check_vma=False,
    )
```
